1024 devices in a mesh: gx: 16 (over z_hi, y), gy: 8 (over x, core), gz: 8 (over z_lo).
Axes of the slice: x: 4, y: 4, z: 32 (z_hi: 4, z_lo: 8; z = z_hi * 8 + z_lo), core: 2. Of those that a mesh axis runs over, the one named last changes fastest.
Arguments:
- conserved: float32 [5, 256, 128, 1024], P(None, 'gx', 'gy', 'gz'), as said below
Outputs:
- advanced: float32 [5, 256, 128, 1024], P(None, 'gx', 'gy', 'gz')
Inputs may be any that keep to these rules, and one draw needn't show every extreme that they name: `conserved`: every cell has positive density and positive pressure (energy above the kinetic energy).
All inputs are finite; a program needn't handle non-finite values. Where the reference program divides by a largest or mean magnitude, that divisor is 1e-20 or more.
Results may differ from the reference program's by a relative error of at most 0.000066.
Values sent between devices are 32-bit elements; how exact they have to be, the bound alone decides.
A program may use at most 32 MiB of HBM per device.

```python
import jax
import jax.numpy as jnp
from jax import lax

NX = 256
NY = 128
NZ = 1024


def draw_conserved(key, part):
    subkeys = jax.random.split(key, 3)
    grid_shape = (NX, NY, NZ)
    log_density = jax.random.uniform(subkeys[0], grid_shape, jnp.float32, -0.7, 0.7)
    log_pressure = jax.random.uniform(subkeys[1], grid_shape, jnp.float32, -0.7, 0.7)
    position = jnp.arange(NX, dtype=jnp.float32) / NX
    vel_scale = (0.3 + 0.6 * position)[:, None, None]
    velocity = jax.random.truncated_normal(subkeys[2], -4.0, 4.0, (3,) + grid_shape, jnp.float32) * vel_scale
    density = jnp.exp(log_density)
    pressure = jnp.exp(log_pressure)
    momentum = density * velocity
    energy = pressure / 0.4 + 0.5 * density * jnp.sum(velocity * velocity, axis=0)
    return jnp.stack([density, momentum[0], momentum[1], momentum[2], energy]).astype(jnp.float32)


def setup_inputs(seed: int = 0) -> dict:
    key_list = jax.random.split(jax.random.key(seed), 2)
    return {
        "conserved": draw_conserved(jax.random.fold_in(key_list[1], 71), 0),
    }


gamma_gas = 1.4
weno_eps = 1e-06
courant = 0.4

def primitives(components):
    density = components[0]
    vel_normal = components[1] / density
    vel_first = components[2] / density
    vel_second = components[3] / density
    kinetic = 0.5 * (vel_normal * vel_normal + vel_first * vel_first + vel_second * vel_second)
    pressure = (gamma_gas - 1.0) * (components[4] - density * kinetic)
    return (density, vel_normal, vel_first, vel_second, kinetic, pressure)

def multiply_rows(matrix, vector):
    result = []
    for matrix_row in matrix:
        accum = None
        for coefficient, component in zip(matrix_row, vector):
            if coefficient is None:
                continue
            product_term = component * coefficient
            accum = product_term if accum is None else accum + product_term
        result.append(accum)
    return result

def weno_face(far_left, near_left, centre, near_right, far_right):
    poly_left = (2.0 * far_left - 7.0 * near_left + 11.0 * centre) / 6.0
    poly_mid = (-near_left + 5.0 * centre + 2.0 * near_right) / 6.0
    poly_right = (2.0 * centre + 5.0 * near_right - far_right) / 6.0
    diff_one = far_left - 2.0 * near_left + centre
    diff_two = far_left - 4.0 * near_left + 3.0 * centre
    smooth_left = 13.0 / 12.0 * diff_one * diff_one + 0.25 * diff_two * diff_two
    diff_one = near_left - 2.0 * centre + near_right
    diff_two = near_left - near_right
    smooth_mid = 13.0 / 12.0 * diff_one * diff_one + 0.25 * diff_two * diff_two
    diff_one = centre - 2.0 * near_right + far_right
    diff_two = 3.0 * centre - 4.0 * near_right + far_right
    smooth_right = 13.0 / 12.0 * diff_one * diff_one + 0.25 * diff_two * diff_two
    weight_left = 0.1 / ((weno_eps + smooth_left) * (weno_eps + smooth_left))
    weight_mid = 0.6 / ((weno_eps + smooth_mid) * (weno_eps + smooth_mid))
    weight_right = 0.3 / ((weno_eps + smooth_right) * (weno_eps + smooth_right))
    return (weight_left * poly_left + weight_mid * poly_mid + weight_right * poly_right) / (weight_left + weight_mid + weight_right)

def face_divergence(components, line_axis, wave_speed, cell_count):
    length = components[0].shape[line_axis] - 6
    face_count = length + 1

    def window(array_item, start, count):
        return lax.slice_in_dim(array_item, start, start + count, axis=line_axis)
    density, vel_normal, vel_first, vel_second, kinetic, pressure = primitives(components)
    fluxes = [components[1], components[1] * vel_normal + pressure, components[2] * vel_normal, components[3] * vel_normal, (components[4] + pressure) * vel_normal]
    split_plus = [0.5 * (flux + wave_speed * component) for flux, component in zip(fluxes, components)]
    split_minus = [0.5 * (flux - wave_speed * component) for flux, component in zip(fluxes, components)]
    face_mean = [0.5 * (window(component, 2, face_count) + window(component, 3, face_count)) for component in components]
    mean_density, mean_normal, mean_first, mean_second, mean_kinetic, mean_pressure = primitives(face_mean)
    enthalpy = (face_mean[4] + mean_pressure) / mean_density
    sound_speed = jnp.sqrt(gamma_gas * mean_pressure / mean_density)
    inv_sound = 1.0 / sound_speed
    coef_one = (gamma_gas - 1.0) / (sound_speed * sound_speed)
    coef_two = coef_one * mean_kinetic
    left_rows = [[0.5 * (coef_two + mean_normal * inv_sound), -0.5 * (coef_one * mean_normal + inv_sound), -0.5 * coef_one * mean_first, -0.5 * coef_one * mean_second, 0.5 * coef_one], [-mean_first, None, 1.0, None, None], [-mean_second, None, None, 1.0, None], [1.0 - coef_two, coef_one * mean_normal, coef_one * mean_first, coef_one * mean_second, -coef_one], [0.5 * (coef_two - mean_normal * inv_sound), -0.5 * (coef_one * mean_normal - inv_sound), -0.5 * coef_one * mean_first, -0.5 * coef_one * mean_second, 0.5 * coef_one]]
    right_cols = [[1.0, None, None, 1.0, 1.0], [mean_normal - sound_speed, None, None, mean_normal, mean_normal + sound_speed], [mean_first, 1.0, None, mean_first, mean_first], [mean_second, None, 1.0, mean_second, mean_second], [enthalpy - mean_normal * sound_speed, mean_first, mean_second, mean_kinetic, enthalpy + mean_normal * sound_speed]]
    positive = [multiply_rows(left_rows, [window(component, offset, face_count) for component in split_plus]) for offset in range(5)]
    negative = [multiply_rows(left_rows, [window(component, offset, face_count) for component in split_minus]) for offset in range(1, 6)]
    wave_sums = []
    for wave_index in range(5):
        upwind = weno_face(*[positive[offset][wave_index] for offset in range(5)])
        downwind = weno_face(*[negative[offset][wave_index] for offset in (4, 3, 2, 1, 0)])
        wave_sums.append(upwind + downwind)
    face_flux = multiply_rows(right_cols, wave_sums)
    return [-(window(flux, 1, length) - window(flux, 0, length)) * cell_count for flux in face_flux]

def component_order(direction):
    if direction == 0:
        return [0, 1, 2, 3, 4]
    if direction == 1:
        return [0, 2, 1, 3, 4]
    return [0, 3, 1, 2, 4]

def direction_terms(padded_slab, line_axis, direction, wave_speed, cell_count):
    comp_order = component_order(direction)
    result = face_divergence([padded_slab[index] for index in comp_order], line_axis, wave_speed, cell_count)
    placed = [None] * 5
    for index, target in enumerate(comp_order):
        placed[target] = result[index]
    return jnp.stack(placed)

def reference(conserved):
    components = [conserved[index] for index in range(5)]
    density, vel_one, vel_two, vel_three, kinetic, pressure = primitives(components)
    sound_speed = jnp.sqrt(gamma_gas * pressure / density)
    speed_x = jnp.max(jnp.abs(vel_one) + sound_speed)
    speed_y = jnp.max(jnp.abs(vel_two) + sound_speed)
    speed_z = jnp.max(jnp.abs(vel_three) + sound_speed)
    step = courant / (speed_x * NX + speed_y * NY + speed_z * NZ)
    padded = jnp.pad(conserved, ((0, 0), (3, 3), (0, 0), (0, 0)), mode='wrap')
    moved = jnp.moveaxis(padded, 2, 0)
    result = lax.map(lambda slab_item: direction_terms(slab_item, 0, 0, speed_x, NX), moved)
    tendency = jnp.moveaxis(result, 0, 2)
    padded = jnp.pad(conserved, ((0, 0), (0, 0), (3, 3), (0, 0)), mode='wrap')
    moved = jnp.moveaxis(padded, 1, 0)
    result = lax.map(lambda slab_item: direction_terms(slab_item, 0, 1, speed_y, NY), moved)
    tendency = tendency + jnp.moveaxis(result, 0, 1)
    padded = jnp.pad(conserved, ((0, 0), (0, 0), (0, 0), (3, 3)), mode='wrap')
    moved = jnp.moveaxis(padded, 1, 0)
    result = lax.map(lambda slab_item: direction_terms(slab_item, 1, 2, speed_z, NZ), moved)
    tendency = tendency + jnp.moveaxis(result, 0, 1)
    return conserved + step * tendency
```

```python
import functools

import jax
import jax.numpy as jnp
from jax import lax
from jax.experimental import pallas as pl
from jax.experimental.pallas import tpu as pltpu
from jax.sharding import PartitionSpec as P

GAMMA = 1.4
COURANT = 0.4
EPS = 1e-06 * 4.0 * 0.75
ORDER = ((0, 1, 2, 3, 4), (0, 2, 1, 3, 4), (0, 3, 1, 2, 4))
MESH = pl.DeviceIdType.MESH
F32 = jnp.float32
ROOTS = 4
Z = 32


def rcp(x):
    return pltpu.reciprocal(x, approx=True)


def rows(start, count=16):
    return pl.ds(pl.multiple_of(start, 8), count)


def flux(q):
    inv = 1.0 / q[0]
    vn = q[1] * inv
    kin2 = (q[1] * q[1] + q[2] * q[2] + q[3] * q[3]) * inv
    p = (GAMMA - 1.0) * (q[4] - 0.5 * kin2)
    return q[1] * vn + p, q[2] * vn, q[3] * vn, (q[4] + p) * vn


def cells(qr, order, dr, lo, hi):
    def body(j, carry):
        q0 = [qr[c, rows(16 * j), :] for c in order]
        q1 = [qr[c, rows(16 * j + 16), :] for c in order]
        f0, f1 = flux(q0), flux(q1)
        for c in range(5):
            dr[c, j] = q1[c] - q0[c]
        for c in range(4):
            dr[5 + c, j] = f1[c] - f0[c]
        return carry

    lax.fori_loop(lo, hi, body, 0)


def faces(qr, order, dr, gh, co, lo, hi):
    def body(f, carry):
        m = [0.5 * (qr[c, rows(16 * f + 32), :] + qr[c, rows(16 * f + 48), :]) for c in order]
        inv = 1.0 / m[0]
        vn, va, vb = m[1] * inv, m[2] * inv, m[3] * inv
        kin = 0.5 * (vn * vn + va * va + vb * vb)
        p = (GAMMA - 1.0) * (m[4] - m[0] * kin)
        c2 = GAMMA * p * inv
        c = jnp.sqrt(c2)
        half_inv_c = 0.5 / c
        half_b1 = (0.5 * (GAMMA - 1.0)) / c2
        for i, v in enumerate((vn, va, vb, kin, c, c2 * (1.0 / (GAMMA - 1.0)))):
            co[f, i] = v
        for k in range(5):
            for w in range(2):
                if w == 0:
                    v = [dr[1, f + k]] + [dr[5 + i, f + k] for i in range(4)]
                else:
                    v = [dr[i, f + k] for i in range(5)]
                a = half_b1 * ((kin * v[0] + v[4]) - (vn * v[1] + va * v[2] + vb * v[3]))
                b = half_inv_c * (v[1] - vn * v[0])
                for i, x in enumerate(
                    (a - b, v[2] - va * v[0], v[3] - vb * v[0], v[0] - (a + a), a + b)
                ):
                    gh[f, 10 * i + 5 * w + k] = x
        return carry

    lax.fori_loop(lo, hi, body, 0)


def base(dr, rb, lo, hi):
    def body(i, carry):
        for c in range(5):
            r = 1 if c == 0 else 4 + c
            d = [dr[r, i + 1 + k] for k in range(4)]
            rb[c, i] = 7.0 * (d[1] + d[2]) - (d[0] + d[3])
            d = [dr[c, i + 1 + k] for k in range(4)]
            rb[5 + c, i] = 3.0 * (d[1] - d[2]) + (d[3] - d[0])
        return carry

    lax.fori_loop(lo, hi, body, 0)


def corr(d1, d2, d3, d4):
    s1, s2, s3 = d2 - d1, d3 - d2, d4 - d3
    a, b = 0.75 * d2, 0.75 * d3
    r0 = rcp(a * (d2 + s1) + (s1 * s1 + EPS))
    r1 = rcp(a * d3 + (s2 * s2 + EPS))
    r2 = rcp(b * (d3 - s3) + (s3 * s3 + EPS))
    w0, w1, w2 = r0 * r0, 6.0 * (r1 * r1), 3.0 * (r2 * r2)
    num = (w0 + w0) * (s1 - s2) + w2 * (s2 - s3)
    return num * rcp(w0 + w1 + w2)


def weno(gh, co, sv, d, fl, lo, hi):
    def body(f, carry):
        s = sv[d]
        kap = []
        for m in range(5):
            g = [gh[f, 10 * m + k] for k in range(5)]
            h = [s * gh[f, 10 * m + 5 + k] for k in range(5)]
            up = corr(g[0] + h[0], g[1] + h[1], g[2] + h[2], g[3] + h[3])
            down = corr(g[4] - h[4], g[3] - h[3], g[2] - h[2], g[1] - h[1])
            kap.append(up - down)
        vn, va, vb, kin, c, e = [co[f, i] for i in range(6)]
        pair = kap[0] + kap[4]
        f0 = pair + kap[3]
        cd = c * (kap[4] - kap[0])
        fl[f, 0] = f0
        fl[f, 1] = vn * f0 + cd
        fl[f, 2] = va * f0 + kap[1]
        fl[f, 3] = vb * f0 + kap[2]
        fl[f, 4] = kin * f0 + e * pair + vn * cd + va * kap[1] + vb * kap[2]
        return carry

    lax.fori_loop(lo, hi, body, 0)


def divergence(rb, fl, sv, d, c, i):
    return sv[3 + d] * (rb[c, i] + sv[d] * rb[5 + c, i] + (fl[i + 1, c] - fl[i, c]))


def kernel(
    counts, q_hbm, out_ref,
    qx, qy, qz, tz, drx, dry, drz, ghx, ghy, ghz, cox, coy, coz, rbx, rby, rbz, flx, fly, flz,
    ay, az, oz, sv, gbuf, ybuf, zbuf, fin, xs, xh, rl, yh, zh_buf,
    in_sem, sg, rg, sy, ry, sz, rz, sb, rbc, s1, r1, s2, r2, s3, r3, sh, rh,
):
    gx, gy, gz = lax.axis_index("gx"), lax.axis_index("gy"), lax.axis_index("gz")
    y, zhi = lax.rem(gx, 4), gx // 4
    z = zhi * 8 + gz

    def in_plane(yy):
        return (zhi * 4 + yy, gy, gz)

    def across(yy, step):
        return (lax.rem(zhi + 4 + step, 4) * 4 + yy, gy, gz)

    def along_z(t):
        return ((t // 8) * 4 + y, gy, lax.rem(t, 8))

    def along_gy(k):
        return (gx, lax.rem(gy + 8 + k, 8), gz)

    def along_gz(k):
        return (gx, gy, lax.rem(gz + 8 + k, 8))

    def remote(src, dst, send, recv, device):
        return pltpu.make_async_remote_copy(
            src_ref=src, dst_ref=dst, send_sem=send, recv_sem=recv, device_id=device, device_id_type=MESH
        )

    load = pltpu.make_async_copy(q_hbm, qx.at[:, pl.ds(48, 256), :], in_sem)
    load.start()

    bar = pltpu.get_barrier_semaphore()

    def tell(device):
        pl.semaphore_signal(bar, inc=1, device_id=device, device_id_type=MESH)

    for k in range(1, 8):
        tell(along_gy(k))
    for k in range(1, 4):
        tell(in_plane(lax.rem(y + k, 4)))
    tell(along_gz(1))
    tell(along_gz(-1))

    @pl.when(y == 0)
    def _():
        for c in range(4):
            tell(across(c, -1))

    @pl.when(y == 3)
    def _():
        for c in range(4):
            tell(across(c, 1))

    @pl.when(z < ROOTS)
    def _():
        def one(k, carry):
            tell(along_z(lax.rem(z + k, Z)))
            return carry

        lax.fori_loop(1, Z, one, 0)

    @pl.when(z >= ROOTS)
    def _():
        tell(along_z(1 + lax.rem(z - ROOTS + 3 * ROOTS, ROOTS - 1)))

    load.wait()

    def speeds(i, carry):
        q = [qx[c, rows(16 * i + 48), :] for c in range(5)]
        inv = 1.0 / q[0]
        v = [q[1] * inv, q[2] * inv, q[3] * inv]
        p = (GAMMA - 1.0) * (q[4] - 0.5 * q[0] * (v[0] * v[0] + v[1] * v[1] + v[2] * v[2]))
        snd = jnp.sqrt(GAMMA * p * inv)
        return tuple(jnp.maximum(m, jnp.abs(u) + snd) for m, u in zip(carry, v))

    zero = jnp.zeros((16, 128), F32)
    lane = lax.broadcasted_iota(jnp.int32, (1, 128), 1)
    local = [jnp.max(jnp.max(m, axis=0, keepdims=True), axis=1, keepdims=True) for m in lax.fori_loop(0, 16, speeds, (zero,) * 3)]
    mine = jnp.where(lane == 0, local[0], jnp.where(lane == 1, local[1], jnp.where(lane == 2, local[2], 0.0)))
    gbuf[0] = mine
    for side, first in ((0, 256), (1, 48)):
        for c in range(4):
            xs[side, c, pl.ds(0, 48), :] = qx[c, pl.ds(first, 48), :]
            xs[side, c, pl.ds(48, 16), :] = qx[4, pl.ds(first + 16 * min(c, 2), 16), :]

    targets = jnp.where(z == 0, 0, jnp.where(z == 1, 10, 9))
    pl.semaphore_wait(bar, 14 + jnp.where(z < ROOTS, ROOTS - 1 + targets, ROOTS))

    def gy_copy(k):
        return remote(gbuf.at[0], gbuf.at[k], sg.at[k], rg.at[k], along_gy(k))

    for k in range(1, 8):
        gy_copy(k).start()

    @pl.when(y == 3)
    def _():
        for c in range(3):
            remote(xs.at[0, c], rl.at[0], s2.at[c], r2.at[0], in_plane(c)).start()

    @pl.when(y == 0)
    def _():
        for c in range(1, 4):
            remote(xs.at[1, c], rl.at[1], s2.at[c], r2.at[1], in_plane(c)).start()

    for k in range(1, 8):
        gy_copy(k).wait_recv()
    ybuf[0] = jnp.max(gbuf[...].reshape(8, 128), axis=0, keepdims=True)

    def y_copy(k):
        return remote(ybuf.at[0], ybuf.at[k], sy.at[k], ry.at[k], in_plane(lax.rem(y + k, 4)))

    for k in range(1, 4):
        y_copy(k).start()
    for k in range(1, 4):
        y_copy(k).wait_recv()
    zbuf[0] = jnp.max(ybuf[...].reshape(4, 128), axis=0, keepdims=True)

    def z_copy(r):
        k = lax.rem(z - r + Z, Z)
        return remote(zbuf.at[0], zbuf.at[k], sz.at[r], rz.at[k], along_z(r))

    for r in range(ROOTS):

        @pl.when(z != r)
        def _(r=r):
            z_copy(r).start()

    def up(src):
        return remote(src, xh.at[0, y], s3.at[0], r3.at[0, y], across(0, 1))

    def down(src):
        return remote(src, xh.at[1, y], s3.at[1], r3.at[1, y], across(3, -1))

    def first_leg(i):
        return remote(xs.at[i, 0], rl.at[i], s2.at[0], r2.at[i], in_plane(y))

    @pl.when(y < 3)
    def _():
        first_leg(0).wait_recv()
        up(rl.at[0]).start()

    @pl.when(y == 3)
    def _():
        up(xs.at[0, 3]).start()

    @pl.when(y > 0)
    def _():
        first_leg(1).wait_recv()
        down(rl.at[1]).start()

    @pl.when(y == 0)
    def _():
        down(xs.at[1, 0]).start()

    def near(i):
        return remote(xs.at[i], xh.at[i], s1.at[i], r1.at[i], in_plane(lax.rem(y + 4 + (1 - 2 * i), 4)))

    @pl.when(y < 3)
    def _():
        near(0).start()

    @pl.when(y > 0)
    def _():
        near(1).start()

    for c in range(5):

        def turn(j, carry, c=c):
            qy[c, rows(16 * j + 48), :] = qx[c, pl.ds(48 + j, 16, stride=16), :]
            return carry

        lax.fori_loop(0, 16, turn, 0)

    def y_halo(i):
        src = qy.at[:, pl.ds(256 if i == 0 else 48, 48), :]
        return remote(src, yh.at[i], sh.at[i], rh.at[i], along_gy(1 - 2 * i))

    y_halo(0).start()
    y_halo(1).start()

    def flip(k, carry):
        block = qx[k // 2, rows(48 + 128 * lax.rem(k, 2), 128), :]
        tz[k, pl.ds(8, 128), :] = block.T
        return carry

    lax.fori_loop(0, 10, flip, 0)

    def z_halo(i):
        src = tz.at[:, pl.ds(128 if i == 0 else 8, 8), :]
        return remote(src, zh_buf.at[i], sh.at[2 + i], rh.at[2 + i], along_gz(1 - 2 * i))

    z_halo(0).start()
    z_halo(1).start()

    cells(qx, ORDER[0], drx, 3, 18)
    faces(qx, ORDER[0], drx, ghx, cox, 3, 14)
    base(drx, rbx, 2, 14)

    y_halo(0).wait_recv()
    y_halo(1).wait_recv()
    qy[:, pl.ds(0, 48), :] = yh[0]
    qy[:, pl.ds(304, 48), :] = yh[1]
    cells(qy, ORDER[1], dry, 0, 21)
    faces(qy, ORDER[1], dry, ghy, coy, 0, 17)
    base(dry, rby, 0, 16)

    z_halo(0).wait_recv()
    z_halo(1).wait_recv()
    z_halo(0).wait_send()
    z_halo(1).wait_send()
    tz[:, pl.ds(5, 3), :] = zh_buf[0, :, pl.ds(5, 3), :]
    tz[:, pl.ds(136, 3), :] = zh_buf[1, :, pl.ds(0, 3), :]
    for c in range(5):

        def line(j, carry, c=c):
            qz[c, rows(16 * j, 8), :] = tz[2 * c, pl.ds(5 + j, 8, stride=16), :]
            qz[c, rows(16 * j + 8, 8), :] = tz[2 * c + 1, pl.ds(5 + j, 8, stride=16), :]
            return carry

        lax.fori_loop(0, 22, line, 0)
    cells(qz, ORDER[2], drz, 0, 21)
    faces(qz, ORDER[2], drz, ghz, coz, 0, 17)
    base(drz, rbz, 0, 16)

    def spread(i):
        t = ROOTS + (ROOTS - 1) * i + z - 1
        return t, remote(fin.at[0], fin.at[1], sb.at[i], rbc.at[0], along_z(lax.rem(t + Z, Z)))

    @pl.when(z < ROOTS)
    def _():
        def arrived(k, carry):
            remote(zbuf.at[0], zbuf.at[k], sz.at[0], rz.at[k], along_z(z)).wait_recv()
            return carry

        lax.fori_loop(1, Z, arrived, 0)
        top = jnp.max(zbuf[...].reshape(Z, 128), axis=0, keepdims=True)
        fin[0] = top
        fin[1] = top

        @pl.when(z > 0)
        def _():
            for i in range(10):
                t, copy = spread(i)

                @pl.when(t < Z)
                def _(copy=copy):
                    copy.start()

    @pl.when(z >= ROOTS)
    def _():
        spread(0)[1].wait_recv()

    row = fin[1]
    s = [jnp.max(jnp.where(lane == d, row, 0.0), axis=1, keepdims=True) for d in range(3)]
    step = COURANT / (s[0] * counts[0] + s[1] * counts[1] + s[2] * counts[2])
    for d in range(3):
        sv[d] = jnp.broadcast_to(s[d], (16, 128))
        sv[3 + d] = jnp.broadcast_to(step * (counts[d] / 12.0), (16, 128))

    weno(ghz, coz, sv, 2, flz, 0, 17)

    def close_z(i, carry):
        for c in range(5):
            az[ORDER[2][c], rows(16 * i), :] = divergence(rbz, flz, sv, 2, c, i)
        return carry

    lax.fori_loop(0, 16, close_z, 0)

    def unflip(k, carry):
        c, half = k // 2, lax.rem(k, 2)
        parts = [az[c, pl.ds(half * 8 + i, 16, stride=16), :] for i in range(8)]
        oz[c, rows(128 * half, 128), :] = jnp.concatenate(parts, axis=0).T
        return carry

    lax.fori_loop(0, 10, unflip, 0)
    weno(ghy, coy, sv, 1, fly, 0, 17)

    def close_y(i, carry):
        for c in range(5):
            ay[ORDER[1][c], rows(16 * i), :] = divergence(rby, fly, sv, 1, c, i)
        return carry

    lax.fori_loop(0, 16, close_y, 0)
    weno(ghx, cox, sv, 0, flx, 3, 14)

    @pl.when(y > 0)
    def _():
        near(0).wait_recv()

    @pl.when(y == 0)
    def _():
        for c in range(4):
            remote(rl.at[0], xh.at[0, c], s3.at[0], r3.at[0, c], across(0, 1)).wait_recv()

    @pl.when(y < 3)
    def _():
        near(1).wait_recv()

    @pl.when(y == 3)
    def _():
        for c in range(4):
            remote(rl.at[0], xh.at[1, c], s3.at[1], r3.at[1, c], across(0, 1)).wait_recv()

    for side, first in ((0, 0), (1, 304)):
        for c in range(4):
            qx[c, pl.ds(first, 48), :] = xh[side, c, pl.ds(0, 48), :]
        for i in range(3):
            qx[4, pl.ds(first + 16 * i, 16), :] = xh[side, i, pl.ds(48, 16), :]
    for lo, hi, flo, fhi in ((0, 3, 0, 3), (18, 21, 14, 17)):
        cells(qx, ORDER[0], drx, lo, hi)
        faces(qx, ORDER[0], drx, ghx, cox, flo, fhi)
        weno(ghx, cox, sv, 0, flx, flo, fhi)
    base(drx, rbx, 0, 2)
    base(drx, rbx, 14, 16)

    def close(i, carry):
        for c in range(5):
            total = divergence(rbx, flx, sv, 0, c, i) + ay[c, pl.ds(i, 16, stride=16), :] + oz[c, rows(16 * i), :]
            out_ref[c, rows(16 * i), :] = qx[c, rows(16 * i + 48), :] - total
        return carry

    lax.fori_loop(0, 16, close, 0)

    for k in range(1, 8):
        gy_copy(k).wait_send()
    for k in range(1, 4):
        y_copy(k).wait_send()
    for r in range(ROOTS):

        @pl.when(z != r)
        def _(r=r):
            z_copy(r).wait_send()

    @pl.when(y == 3)
    def _():
        for c in range(3):
            remote(xs.at[0, c], rl.at[0], s2.at[c], r2.at[0], in_plane(c)).wait_send()

    @pl.when(y == 0)
    def _():
        for c in range(1, 4):
            remote(xs.at[1, c], rl.at[1], s2.at[c], r2.at[1], in_plane(c)).wait_send()

    up(rl.at[0]).wait_send()
    down(rl.at[1]).wait_send()

    @pl.when(y < 3)
    def _():
        near(0).wait_send()

    @pl.when(y > 0)
    def _():
        near(1).wait_send()

    y_halo(0).wait_send()
    y_halo(1).wait_send()

    @pl.when(jnp.logical_and(z > 0, z < ROOTS))
    def _():
        for i in range(10):
            t, copy = spread(i)

            @pl.when(t < Z)
            def _(copy=copy):
                copy.wait_send()


def per_device(conserved):
    counts = [
        float(n * lax.axis_size(a)) for n, a in zip(conserved.shape[1:], ("gx", "gy", "gz"))
    ]
    vm = lambda *shape: pltpu.VMEM(shape, F32)
    dma = lambda *shape: pltpu.SemaphoreType.DMA(shape)
    scratch = (
        [vm(5, 352, 128)] * 3 + [vm(10, 144, 128)] + [vm(9, 21, 16, 128)] * 3
        + [vm(17, 50, 16, 128)] * 3 + [vm(17, 6, 16, 128)] * 3 + [vm(10, 16, 16, 128)] * 3
        + [vm(17, 5, 16, 128)] * 3 + [vm(5, 256, 128)] * 3 + [vm(6, 16, 128)]
        + [vm(8, 1, 128), vm(4, 1, 128), vm(Z, 1, 128), vm(2, 1, 128)]
        + [vm(2, 4, 64, 128), vm(2, 4, 64, 128), vm(2, 64, 128), vm(2, 5, 48, 128), vm(2, 10, 8, 128)]
        + [pltpu.SemaphoreType.DMA, dma(8), dma(8), dma(4), dma(4), dma(ROOTS), dma(Z), dma(10), dma(1)]
        + [dma(2), dma(2), dma(4), dma(2), dma(2), dma(2, 4), dma(4), dma(4)]
    )
    flat = conserved.reshape(5, 256, 128)
    out = pl.pallas_call(
        functools.partial(kernel, counts),
        out_shape=jax.ShapeDtypeStruct(flat.shape, F32),
        in_specs=[pl.BlockSpec(memory_space=pl.ANY)],
        out_specs=pl.BlockSpec(memory_space=pltpu.VMEM),
        scratch_shapes=scratch,
        compiler_params=pltpu.CompilerParams(
            collective_id=0, has_side_effects=True, vmem_limit_bytes=60 * 2**20
        ),
        name="weno_section",
    )(flat)
    return out.reshape(conserved.shape)


def solution(mesh):
    spec = P(None, "gx", "gy", "gz")
    return jax.shard_map(
        per_device, mesh=mesh, in_specs=(spec,), out_specs=spec, check_vma=False
    )
```

```python
import functools

import jax
import jax.numpy as jnp
from jax import lax
from jax.experimental import pallas as pl
from jax.experimental.pallas import tpu as pltpu
from jax.sharding import PartitionSpec as P

GAMMA = 1.4
COURANT = 0.4
EPS = 1e-06 * 4.0 * 0.75
ORDER = ((0, 1, 2, 3, 4), (0, 2, 1, 3, 4), (0, 3, 1, 2, 4))
MESH = pl.DeviceIdType.MESH
F32 = jnp.float32
ROOTS = 4
Z = 32


def rcp(x):
    return pltpu.reciprocal(x, approx=True)


def rows(start, count=16):
    return pl.ds(pl.multiple_of(start, 8), count)


def flux(q):
    inv = 1.0 / q[0]
    vn = q[1] * inv
    kin2 = (q[1] * q[1] + q[2] * q[2] + q[3] * q[3]) * inv
    p = (GAMMA - 1.0) * (q[4] - 0.5 * kin2)
    return q[1] * vn + p, q[2] * vn, q[3] * vn, (q[4] + p) * vn


def cells(qr, order, dr, lo, hi):
    def body(j, carry):
        q0 = [qr[c, rows(16 * j), :] for c in order]
        q1 = [qr[c, rows(16 * j + 16), :] for c in order]
        f0, f1 = flux(q0), flux(q1)
        for c in range(5):
            dr[c, j] = q1[c] - q0[c]
        for c in range(4):
            dr[5 + c, j] = f1[c] - f0[c]
        return carry

    lax.fori_loop(lo, hi, body, 0)


def faces(qr, order, dr, gh, co, lo, hi):
    def body(f, carry):
        m = [0.5 * (qr[c, rows(16 * f + 32), :] + qr[c, rows(16 * f + 48), :]) for c in order]
        inv = 1.0 / m[0]
        vn, va, vb = m[1] * inv, m[2] * inv, m[3] * inv
        kin = 0.5 * (vn * vn + va * va + vb * vb)
        p = (GAMMA - 1.0) * (m[4] - m[0] * kin)
        c2 = GAMMA * p * inv
        c = jnp.sqrt(c2)
        half_inv_c = 0.5 / c
        half_b1 = (0.5 * (GAMMA - 1.0)) / c2
        for i, v in enumerate((vn, va, vb, kin, c, c2 * (1.0 / (GAMMA - 1.0)))):
            co[f, i] = v
        for k in range(5):
            for w in range(2):
                if w == 0:
                    v = [dr[1, f + k]] + [dr[5 + i, f + k] for i in range(4)]
                else:
                    v = [dr[i, f + k] for i in range(5)]
                a = half_b1 * ((kin * v[0] + v[4]) - (vn * v[1] + va * v[2] + vb * v[3]))
                b = half_inv_c * (v[1] - vn * v[0])
                for i, x in enumerate(
                    (a - b, v[2] - va * v[0], v[3] - vb * v[0], v[0] - (a + a), a + b)
                ):
                    gh[f, 10 * i + 5 * w + k] = x
        return carry

    lax.fori_loop(lo, hi, body, 0)


def base(dr, rb, lo, hi):
    def body(i, carry):
        for c in range(5):
            r = 1 if c == 0 else 4 + c
            d = [dr[r, i + 1 + k] for k in range(4)]
            rb[c, i] = 7.0 * (d[1] + d[2]) - (d[0] + d[3])
            d = [dr[c, i + 1 + k] for k in range(4)]
            rb[5 + c, i] = 3.0 * (d[1] - d[2]) + (d[3] - d[0])
        return carry

    lax.fori_loop(lo, hi, body, 0)


def corr(d1, d2, d3, d4):
    s1, s2, s3 = d2 - d1, d3 - d2, d4 - d3
    a, b = 0.75 * d2, 0.75 * d3
    r0 = rcp(a * (d2 + s1) + (s1 * s1 + EPS))
    r1 = rcp(a * d3 + (s2 * s2 + EPS))
    r2 = rcp(b * (d3 - s3) + (s3 * s3 + EPS))
    w0, w1, w2 = r0 * r0, 6.0 * (r1 * r1), 3.0 * (r2 * r2)
    num = (w0 + w0) * (s1 - s2) + w2 * (s2 - s3)
    return num * rcp(w0 + w1 + w2)


def weno(gh, co, sv, d, fl, lo, hi, also=None):
    def body(f, carry):
        if also is not None:
            also(f)
        s = sv[d]
        kap = []
        for m in range(5):
            g = [gh[f, 10 * m + k] for k in range(5)]
            h = [s * gh[f, 10 * m + 5 + k] for k in range(5)]
            up = corr(g[0] + h[0], g[1] + h[1], g[2] + h[2], g[3] + h[3])
            down = corr(g[4] - h[4], g[3] - h[3], g[2] - h[2], g[1] - h[1])
            kap.append(up - down)
        vn, va, vb, kin, c, e = [co[f, i] for i in range(6)]
        pair = kap[0] + kap[4]
        f0 = pair + kap[3]
        cd = c * (kap[4] - kap[0])
        fl[f, 0] = f0
        fl[f, 1] = vn * f0 + cd
        fl[f, 2] = va * f0 + kap[1]
        fl[f, 3] = vb * f0 + kap[2]
        fl[f, 4] = kin * f0 + e * pair + vn * cd + va * kap[1] + vb * kap[2]
        return carry

    lax.fori_loop(lo, hi, body, 0)


def divergence(rb, fl, sv, d, c, i):
    return sv[3 + d] * (rb[c, i] + sv[d] * rb[5 + c, i] + (fl[i + 1, c] - fl[i, c]))


def kernel(
    counts, q_hbm, out_ref,
    qx, qy, qz, tz, drx, dry, drz, ghx, ghy, ghz, cox, coy, coz, rbx, rby, rbz, flx, fly, flz,
    ay, az, oz, sv, gbuf, zbuf, fin, xs, xh, rl, yh, zh_buf,
    in_sem, sg, rg, sz, rz, sb, rbc, s1, r1, s2, r2, s3, r3, sh, rh,
):
    gx, gy, gz = lax.axis_index("gx"), lax.axis_index("gy"), lax.axis_index("gz")
    y, zhi = lax.rem(gx, 4), gx // 4
    z = zhi * 8 + gz

    def in_plane(yy):
        return (zhi * 4 + yy, gy, gz)

    def across(yy, step):
        return (lax.rem(zhi + 4 + step, 4) * 4 + yy, gy, gz)

    def along_z(t):
        return ((t // 8) * 4 + y, gy, lax.rem(t, 8))

    def at(yy, t):
        return ((t // 8) * 4 + yy, gy, lax.rem(t, 8))

    def along_gy(k):
        return (gx, lax.rem(gy + 8 + k, 8), gz)

    def along_gz(k):
        return (gx, gy, lax.rem(gz + 8 + k, 8))

    def remote(src, dst, send, recv, device):
        return pltpu.make_async_remote_copy(
            src_ref=src, dst_ref=dst, send_sem=send, recv_sem=recv, device_id=device, device_id_type=MESH
        )

    load = pltpu.make_async_copy(q_hbm, qx.at[:, pl.ds(48, 256), :], in_sem)
    load.start()

    bar = pltpu.get_barrier_semaphore()

    def tell(device):
        pl.semaphore_signal(bar, inc=1, device_id=device, device_id_type=MESH)

    for k in range(1, 8):
        tell(along_gy(k))
    for k in range(1, 4):
        tell(in_plane(lax.rem(y + k, 4)))
    tell(along_gz(1))
    tell(along_gz(-1))

    @pl.when(y == 0)
    def _():
        for c in range(4):
            tell(across(c, -1))

    @pl.when(y == 3)
    def _():
        for c in range(4):
            tell(across(c, 1))

    @pl.when(z < ROOTS)
    def _():
        def one(k, carry):
            tell(at(lax.rem(y + k, 4), lax.rem(z + k // 4, Z)))
            return carry

        lax.fori_loop(4, 4 * Z, one, 0)

    @pl.when(z >= ROOTS)
    def _():
        tell(along_z(1 + lax.rem(z - ROOTS + 3 * ROOTS, ROOTS - 1)))

    load.wait()

    def speeds(i, carry):
        q = [qx[c, rows(16 * i + 48), :] for c in range(5)]
        inv = 1.0 / q[0]
        v = [q[1] * inv, q[2] * inv, q[3] * inv]
        p = (GAMMA - 1.0) * (q[4] - 0.5 * q[0] * (v[0] * v[0] + v[1] * v[1] + v[2] * v[2]))
        snd = jnp.sqrt(GAMMA * p * inv)
        return tuple(jnp.maximum(m, jnp.abs(u) + snd) for m, u in zip(carry, v))

    zero = jnp.zeros((16, 128), F32)
    lane = lax.broadcasted_iota(jnp.int32, (1, 128), 1)
    local = [jnp.max(jnp.max(m, axis=0, keepdims=True), axis=1, keepdims=True) for m in lax.fori_loop(0, 16, speeds, (zero,) * 3)]
    mine = jnp.where(lane == 0, local[0], jnp.where(lane == 1, local[1], jnp.where(lane == 2, local[2], 0.0)))
    gbuf[0] = mine
    for side, first in ((0, 256), (1, 48)):
        for c in range(4):
            xs[side, c, pl.ds(0, 48), :] = qx[c, pl.ds(first, 48), :]
            xs[side, c, pl.ds(48, 16), :] = qx[4, pl.ds(first + 16 * min(c, 2), 16), :]

    targets = jnp.where(z == 0, 0, jnp.where(z == 1, 10, 9))
    pl.semaphore_wait(bar, 14 + jnp.where(z < ROOTS, 4 * (ROOTS - 1) + targets, 4 * ROOTS))

    def gy_copy(k):
        return remote(gbuf.at[0], gbuf.at[k], sg.at[k], rg.at[k], along_gy(k))

    for k in range(1, 8):
        gy_copy(k).start()

    @pl.when(y == 3)
    def _():
        for c in range(3):
            remote(xs.at[0, c], rl.at[0], s2.at[c], r2.at[0], in_plane(c)).start()

    @pl.when(y == 0)
    def _():
        for c in range(1, 4):
            remote(xs.at[1, c], rl.at[1], s2.at[c], r2.at[1], in_plane(c)).start()

    for k in range(1, 8):
        gy_copy(k).wait_recv()
    zbuf[0] = jnp.max(gbuf[...], axis=0)

    def z_copy(r, k):
        slot = 4 * lax.rem(z - r + Z, Z) + (4 - k) % 4
        return remote(zbuf.at[0], zbuf.at[slot], sz.at[4 * r + k], rz.at[0], at(lax.rem(y + k, 4), r))

    for r in range(ROOTS):
        for k in range(1, 4):
            z_copy(r, k).start()

        @pl.when(z != r)
        def _(r=r):
            z_copy(r, 0).start()

    def up(src):
        return remote(src, xh.at[0, y], s3.at[0], r3.at[0, y], across(0, 1))

    def down(src):
        return remote(src, xh.at[1, y], s3.at[1], r3.at[1, y], across(3, -1))

    def first_leg(i):
        return remote(xs.at[i, 0], rl.at[i], s2.at[0], r2.at[i], in_plane(y))

    def near(i):
        return remote(xs.at[i], xh.at[i], s1.at[i], r1.at[i], in_plane(lax.rem(y + 4 + (1 - 2 * i), 4)))

    @pl.when(y < 3)
    def _():
        near(0).start()

    @pl.when(y > 0)
    def _():
        near(1).start()

    for c in range(5):

        def turn(j, carry, c=c):
            qy[c, rows(16 * j + 48), :] = qx[c, pl.ds(48 + j, 16, stride=16), :]
            return carry

        lax.fori_loop(0, 16, turn, 0)

    def y_halo(i):
        src = qy.at[:, pl.ds(256 if i == 0 else 48, 48), :]
        return remote(src, yh.at[i], sh.at[i], rh.at[i], along_gy(1 - 2 * i))

    y_halo(0).start()
    y_halo(1).start()

    def flip(k, carry):
        block = qx[k // 2, rows(48 + 128 * lax.rem(k, 2), 128), :]
        tz[k, pl.ds(8, 128), :] = block.T
        return carry

    lax.fori_loop(0, 10, flip, 0)

    def z_halo(i):
        src = tz.at[:, pl.ds(128 if i == 0 else 8, 8), :]
        return remote(src, zh_buf.at[i], sh.at[2 + i], rh.at[2 + i], along_gz(1 - 2 * i))

    z_halo(0).start()
    z_halo(1).start()

    @pl.when(y < 3)
    def _():
        first_leg(0).wait_recv()
        up(rl.at[0]).start()

    @pl.when(y == 3)
    def _():
        up(xs.at[0, 3]).start()

    @pl.when(y > 0)
    def _():
        first_leg(1).wait_recv()
        down(rl.at[1]).start()

    @pl.when(y == 0)
    def _():
        down(xs.at[1, 0]).start()

    cells(qx, ORDER[0], drx, 3, 18)
    faces(qx, ORDER[0], drx, ghx, cox, 3, 14)
    base(drx, rbx, 2, 14)

    y_halo(0).wait_recv()
    y_halo(1).wait_recv()
    qy[:, pl.ds(0, 48), :] = yh[0]
    qy[:, pl.ds(304, 48), :] = yh[1]
    cells(qy, ORDER[1], dry, 0, 21)
    faces(qy, ORDER[1], dry, ghy, coy, 0, 17)
    base(dry, rby, 0, 16)

    z_halo(0).wait_recv()
    z_halo(1).wait_recv()
    z_halo(0).wait_send()
    z_halo(1).wait_send()
    tz[:, pl.ds(5, 3), :] = zh_buf[0, :, pl.ds(5, 3), :]
    tz[:, pl.ds(136, 3), :] = zh_buf[1, :, pl.ds(0, 3), :]
    for c in range(5):

        def line(j, carry, c=c):
            qz[c, rows(16 * j, 8), :] = tz[2 * c, pl.ds(5 + j, 8, stride=16), :]
            qz[c, rows(16 * j + 8, 8), :] = tz[2 * c + 1, pl.ds(5 + j, 8, stride=16), :]
            return carry

        lax.fori_loop(0, 22, line, 0)
    cells(qz, ORDER[2], drz, 0, 21)
    faces(qz, ORDER[2], drz, ghz, coz, 0, 17)
    base(drz, rbz, 0, 16)

    def spread(i):
        t = ROOTS + (ROOTS - 1) * i + z - 1
        return t, remote(fin.at[0], fin.at[1], sb.at[i], rbc.at[0], along_z(lax.rem(t + Z, Z)))

    @pl.when(z < ROOTS)
    def _():
        others = zbuf.at[pl.ds(1, 4 * Z - 1)]
        remote(others, others, sz.at[0], rz.at[0], along_z(z)).wait_recv()
        top = jnp.max(zbuf[...], axis=0)
        fin[0] = top
        fin[1] = top

        @pl.when(z > 0)
        def _():
            for i in range(10):
                t, copy = spread(i)

                @pl.when(t < Z)
                def _(copy=copy):
                    copy.start()

    @pl.when(z >= ROOTS)
    def _():
        spread(0)[1].wait_recv()

    row = fin[1]
    s = [jnp.max(jnp.where(lane == d, row, 0.0), axis=1, keepdims=True) for d in range(3)]
    step = COURANT / (s[0] * counts[0] + s[1] * counts[1] + s[2] * counts[2])
    for d in range(3):
        sv[d] = jnp.broadcast_to(s[d], (16, 128))
        sv[3 + d] = jnp.broadcast_to(step * (counts[d] / 12.0), (16, 128))

    weno(ghz, coz, sv, 2, flz, 0, 17)

    def close_z(i, carry):
        for c in range(5):
            az[ORDER[2][c], rows(16 * i), :] = divergence(rbz, flz, sv, 2, c, i)
        return carry

    lax.fori_loop(0, 16, close_z, 0)

    def unflip(k):
        c, half = k // 2, lax.rem(k, 2)
        parts = [az[c, pl.ds(half * 8 + i, 16, stride=16), :] for i in range(8)]
        oz[c, rows(128 * half, 128), :] = jnp.concatenate(parts, axis=0).T

    weno(ghy, coy, sv, 1, fly, 0, 10, unflip)
    weno(ghy, coy, sv, 1, fly, 10, 17)

    def close_y(i, carry):
        for c in range(5):
            ay[ORDER[1][c], rows(16 * i), :] = divergence(rby, fly, sv, 1, c, i)
        return carry

    lax.fori_loop(0, 16, close_y, 0)
    weno(ghx, cox, sv, 0, flx, 3, 14)

    @pl.when(y > 0)
    def _():
        near(0).wait_recv()

    @pl.when(y == 0)
    def _():
        for c in range(4):
            remote(rl.at[0], xh.at[0, c], s3.at[0], r3.at[0, c], across(0, 1)).wait_recv()

    @pl.when(y < 3)
    def _():
        near(1).wait_recv()

    @pl.when(y == 3)
    def _():
        for c in range(4):
            remote(rl.at[0], xh.at[1, c], s3.at[1], r3.at[1, c], across(0, 1)).wait_recv()

    for side, first in ((0, 0), (1, 304)):
        for c in range(4):
            qx[c, pl.ds(first, 48), :] = xh[side, c, pl.ds(0, 48), :]
        for i in range(3):
            qx[4, pl.ds(first + 16 * i, 16), :] = xh[side, i, pl.ds(48, 16), :]
    for lo, hi, flo, fhi in ((0, 3, 0, 3), (18, 21, 14, 17)):
        cells(qx, ORDER[0], drx, lo, hi)
        faces(qx, ORDER[0], drx, ghx, cox, flo, fhi)
        weno(ghx, cox, sv, 0, flx, flo, fhi)
    base(drx, rbx, 0, 2)
    base(drx, rbx, 14, 16)

    def close(i, carry):
        for c in range(5):
            total = divergence(rbx, flx, sv, 0, c, i) + ay[c, pl.ds(i, 16, stride=16), :] + oz[c, rows(16 * i), :]
            out_ref[c, rows(16 * i), :] = qx[c, rows(16 * i + 48), :] - total
        return carry

    lax.fori_loop(0, 16, close, 0)

    for k in range(1, 8):
        gy_copy(k).wait_send()
    for r in range(ROOTS):
        for k in range(1, 4):
            z_copy(r, k).wait_send()

        @pl.when(z != r)
        def _(r=r):
            z_copy(r, 0).wait_send()

    @pl.when(y == 3)
    def _():
        for c in range(3):
            remote(xs.at[0, c], rl.at[0], s2.at[c], r2.at[0], in_plane(c)).wait_send()

    @pl.when(y == 0)
    def _():
        for c in range(1, 4):
            remote(xs.at[1, c], rl.at[1], s2.at[c], r2.at[1], in_plane(c)).wait_send()

    up(rl.at[0]).wait_send()
    down(rl.at[1]).wait_send()

    @pl.when(y < 3)
    def _():
        near(0).wait_send()

    @pl.when(y > 0)
    def _():
        near(1).wait_send()

    y_halo(0).wait_send()
    y_halo(1).wait_send()

    @pl.when(jnp.logical_and(z > 0, z < ROOTS))
    def _():
        for i in range(10):
            t, copy = spread(i)

            @pl.when(t < Z)
            def _(copy=copy):
                copy.wait_send()


def per_device(conserved):
    counts = [
        float(n * lax.axis_size(a)) for n, a in zip(conserved.shape[1:], ("gx", "gy", "gz"))
    ]
    vm = lambda *shape: pltpu.VMEM(shape, F32)
    dma = lambda *shape: pltpu.SemaphoreType.DMA(shape)
    scratch = (
        [vm(5, 352, 128)] * 3 + [vm(10, 144, 128)] + [vm(9, 21, 16, 128)] * 3
        + [vm(17, 50, 16, 128)] * 3 + [vm(17, 6, 16, 128)] * 3 + [vm(10, 16, 16, 128)] * 3
        + [vm(17, 5, 16, 128)] * 3 + [vm(5, 256, 128)] * 3 + [vm(6, 16, 128)]
        + [vm(8, 1, 128), vm(4 * Z, 1, 128), vm(2, 1, 128)]
        + [vm(2, 4, 64, 128), vm(2, 4, 64, 128), vm(2, 64, 128), vm(2, 5, 48, 128), vm(2, 10, 8, 128)]
        + [pltpu.SemaphoreType.DMA, dma(8), dma(8), dma(4 * ROOTS), dma(1), dma(10), dma(1)]
        + [dma(2), dma(2), dma(4), dma(2), dma(2), dma(2, 4), dma(4), dma(4)]
    )
    flat = conserved.reshape(5, 256, 128)
    out = pl.pallas_call(
        functools.partial(kernel, counts),
        out_shape=jax.ShapeDtypeStruct(flat.shape, F32),
        in_specs=[pl.BlockSpec(memory_space=pl.ANY)],
        out_specs=pl.BlockSpec(memory_space=pltpu.VMEM),
        scratch_shapes=scratch,
        compiler_params=pltpu.CompilerParams(
            collective_id=0, has_side_effects=True, vmem_limit_bytes=48 * 2**20
        ),
        name="weno_section",
    )(pltpu.with_memory_space_constraint(flat, pltpu.HBM))
    return out.reshape(conserved.shape)


def solution(mesh):
    spec = P(None, "gx", "gy", "gz")
    return jax.shard_map(
        per_device, mesh=mesh, in_specs=(spec,), out_specs=spec, check_vma=False
    )
```
